32 devices in a mesh: adapter: 8 (over z, y), tensor: 4 (over x, core).
Axes of the slice: x: 2, y: 2, z: 4, core: 2. Of those that a mesh axis runs over, the one named last changes fastest.
Arguments:
- hidden: bfloat16 [256, 4096], P('adapter', 'tensor'), may hold values from -6 to 6
- request_adapter: int32 [256, 1], P('adapter'), may hold values from 0 to 15; in each aligned block of 32 rows (0 to 31, 32 to 63, ...) at most 2 rows name the same one
- adapter_table_row: int32 [16], replicated, may hold values from 0 to 15, each once
- query_base_weight: bfloat16 [4096, 4096], P(None, 'tensor'), may hold values from -0.09375 to 0.09375
- down_weight: bfloat16 [16, 4096, 16], P('adapter'), may hold values from -0.09375 to 0.09375
- up_weight: bfloat16 [16, 16, 4096], P('adapter', None, 'tensor'), may hold values from -1.5 to 1.5
- column_scale: bfloat16 [16, 4096], P('adapter', 'tensor'), may hold values from 0.5 to 2
- rotated_key_cache: bfloat16 [256, 512, 1024], P('adapter', None, 'tensor'), may hold values from -600 to 600
- cached_value_rows: bfloat16 [256, 512, 1024], P('adapter', None, 'tensor'), may hold values from -6 to 6
- cache_lengths: int32 [256], P('adapter'), may hold values from 64 to 512
Outputs:
- attention: bfloat16 [256, 4096], P('adapter', 'tensor')
The draws below stay inside these ranges and needn't reach their ends.
Inputs may be any that keep to these rules, and one draw needn't show every extreme that they name: `request_adapter`: among the requests of one device, at most 2 use the same adapter. `adapter_table_row`: A permutation. Table row r is held by index r // 2 of the adapter axis.
All inputs are finite; a program needn't handle non-finite values.
Results may differ from the reference program's by a relative error of at most 0.022.
Values may be sent and summed in bfloat16 or wider, within the bound.
A program may use at most 64 MiB of HBM per device.

```python
import math
import jax
import jax.numpy as jnp
import numpy as np
from jax import lax

MODEL_WIDTH = 4096
QUERY_HEADS = 32
KV_HEADS = 8
HEAD_SIZE = 128
ADAPTER_RANK = 16
CAP = 2
REQ_DEV = 32
CTX = 512
ADAPTER_TOTAL = 16
REQUESTS = 256


def draw_rotated_key_cache(key, part):
    normal_key = jax.random.fold_in(jax.random.fold_in(key, 11), 0)
    values = jnp.clip(jax.random.normal(normal_key, (REQUESTS, CTX, KV_HEADS * HEAD_SIZE), jnp.float32), -4.0, 4.0)
    return values.astype(jnp.bfloat16)


def place_ends(result, rng, least, high):
    index_at = [jax.random.randint(jax.random.fold_in(rng, axis), (), 0, length) for axis, length in enumerate(result.shape)]
    longest = result.shape.index(max(result.shape))
    next_to = index_at[:longest] + [(index_at[longest] + 1) % result.shape[longest]] + index_at[longest + 1:]
    return result.at[tuple(index_at)].set(least).at[tuple(next_to)].set(high)


def levels(stream_key, dims, cuts, smallest, top_value):
    level, own = 1.0, jax.random.fold_in(stream_key, 6)
    for dim, shards_of in cuts:
        heights = jnp.exp(jax.random.uniform(jax.random.fold_in(own, dim), (shards_of,), jnp.float32, smallest / len(cuts), top_value / len(cuts)))
        level = level * jnp.repeat(heights, dims[dim] // shards_of).reshape([-1 if axis == dim else 1 for axis in range(len(dims))])
    return level


def assign_block(stream_key, own, number, rows, amount, top, limit, lean):
    order = jax.random.permutation(stream_key, amount)
    crowded, ordinary = load_shares(amount, rows * top, limit, lean, True), load_shares(amount, rows * top, limit, lean, False)
    places = jnp.arange(amount)

    def named(sizes, rotation):
        used = int((sizes > 0).sum())
        fixed = max(1, used // 4)
        shifted = fixed + (places - fixed + rotation * (used - fixed)) % max(1, amount - fixed)
        return jnp.zeros((amount,), jnp.int32).at[order[jnp.where(places < fixed, places, shifted)]].set(jnp.asarray(sizes, jnp.int32))

    sizes = jnp.where(number % 4 == 0, named(crowded, number // 4), named(ordinary, number - number // 4 - 1))
    mixed = jax.random.permutation(jax.random.fold_in(own, 3), amount)
    source_of, sink = mixed[0:amount // 2 * 2:2], mixed[1:amount // 2 * 2:2]
    slack = jnp.minimum(sizes[source_of] - 1, limit - sizes[sink]) // 2
    slack = jnp.where((source_of == order[0]) | (sink == order[0]) | (sizes[sink] == 0), 0, jnp.maximum(slack, 0))
    shifted = jax.random.randint(jax.random.fold_in(own, 4), (amount // 2,), 0, 1 << 20) % (slack + 1)
    sizes = sizes.at[source_of].add(-shifted).at[sink].add(shifted)
    labels = jnp.searchsorted(jnp.cumsum(sizes), jnp.arange(rows * top), side="right").astype(jnp.int32)
    table = labels.reshape(top, rows).T
    table = table[jax.random.permutation(jax.random.fold_in(own, 1), rows)]
    rotation = jax.random.randint(jax.random.fold_in(own, 2), (rows, 1), 0, top)
    return jnp.take_along_axis(table, (jnp.arange(top)[None, :] + rotation) % top, axis=1)


def load_shares(count, total, most, slope, full):
    loads = [(1 << 20) // math.isqrt(grade ** slope) + 1 for grade in range(1, count + 1)]
    largest = most if full else min(most, max(-(-total // count), total * loads[0] // sum(loads)))
    least = 1 if total - largest >= count - 1 else 0
    given, spare = [largest] + [least] * (count - 1), total - largest - least * (count - 1)
    while spare > 0:
        candidates = [i for i in range(1, count) if given[i] < largest] or [i for i in range(1, count) if given[i] < most]
        mass, remaining = sum([loads[i] for i in candidates]), spare
        for i in candidates:
            more = min(most - given[i], max(1, remaining * loads[i] // mass), spare)
            given[i] = given[i] + more
            spare = spare - more
    return np.array(given)


def gaussian(rng, dims, spread, limit, cuts=(), held_as=jnp.bfloat16):
    array = spread * jax.random.normal(rng, dims, jnp.float32)
    if cuts:
        array = array * levels(rng, dims, cuts, -0.22, 0.18)
    return jnp.clip(array, -limit, limit).astype(held_as)


def setup_inputs(seed: int = 0) -> dict:
    seeds = jax.random.split(jax.random.key(seed), 11)
    hidden = gaussian(seeds[0], (REQUESTS, MODEL_WIDTH), 1.0, 6.0, ((0, 8), (1, 4)))
    request_adapter_keys = jax.random.split(jax.random.fold_in(seeds[1], 1), REQUESTS // REQ_DEV)
    request_adapter_turns = jax.random.permutation(jax.random.fold_in(seeds[1], 3), REQUESTS // REQ_DEV)
    request_adapter = jax.vmap(lambda own, number: assign_block(jax.random.fold_in(seeds[1], 2), own, number, REQ_DEV, ADAPTER_TOTAL, 1, CAP, 2))(request_adapter_keys, request_adapter_turns).reshape((REQUESTS, 1))
    adapter_table_row = jax.random.permutation(seeds[2], ADAPTER_TOTAL).astype(jnp.int32)
    query_base_weight = gaussian(seeds[3], (MODEL_WIDTH, QUERY_HEADS * HEAD_SIZE), MODEL_WIDTH ** -0.5, 0.09375, ((1, 4),))
    down_weight = gaussian(seeds[4], (ADAPTER_TOTAL, MODEL_WIDTH, ADAPTER_RANK), MODEL_WIDTH ** -0.5, 0.09375, ((0, 8),))
    up_weight = gaussian(seeds[5], (ADAPTER_TOTAL, ADAPTER_RANK, QUERY_HEADS * HEAD_SIZE), ADAPTER_RANK ** -0.5, 1.5, ((0, 8), (2, 4)))
    column_scale = jnp.clip(jnp.exp(math.log(2.0) - 1.3862944 * jax.random.uniform(seeds[6], (ADAPTER_TOTAL, QUERY_HEADS * HEAD_SIZE), jnp.float32) ** levels(seeds[6], (ADAPTER_TOTAL, QUERY_HEADS * HEAD_SIZE), ((0, 8), (1, 4)), -0.2, 0.2)), 0.5, 2.0).astype(jnp.bfloat16)
    rotated_key_cache = draw_rotated_key_cache(jax.random.fold_in(seeds[10], 71), 0)
    cached_value_rows = gaussian(seeds[8], (REQUESTS, CTX, KV_HEADS * HEAD_SIZE), 1.0, 6.0, ((0, 8), (2, 4)))
    cache_lengths = place_ends(jax.random.randint(seeds[9], (REQUESTS,), CTX // 8, CTX + 1), jax.random.fold_in(seeds[9], 1), CTX // 8, CTX).astype(jnp.int32)
    return {"hidden": hidden, "request_adapter": request_adapter, "adapter_table_row": adapter_table_row, "query_base_weight": query_base_weight, "down_weight": down_weight, "up_weight": up_weight, "column_scale": column_scale, "rotated_key_cache": rotated_key_cache, "cached_value_rows": cached_value_rows, "cache_lengths": cache_lengths}


ROPE_BASE = 500000.0


def rotate(queries, lengths):
    half_size = HEAD_SIZE // 2
    frequency = ROPE_BASE ** (-(jnp.arange(half_size, dtype=jnp.float32) * 2.0) / HEAD_SIZE)
    angles = (lengths - 1).astype(jnp.float32)[:, None] * frequency[None, :]
    cosine = jnp.cos(angles)[:, None, :]
    sine_part = jnp.sin(angles)[:, None, :]
    front_half = queries[..., :half_size]
    back_half = queries[..., half_size:]
    return jnp.concatenate([front_half * cosine - back_half * sine_part, back_half * cosine + front_half * sine_part], axis=-1)


def attend_one(item):
    grouped_row, key_rows, value_rows, length = item
    scores = jnp.einsum('kgd,tkd->kgt', grouped_row.astype(jnp.float32), key_rows.astype(jnp.float32)) * (HEAD_SIZE ** -0.5)
    valid = jnp.arange(CTX, dtype=jnp.int32) < length
    scores = jnp.where(valid[None, None, :], scores, -1e30)
    highest = jnp.max(scores, axis=-1, keepdims=True)
    weights = jnp.where(valid[None, None, :], jnp.exp(scores - highest), 0.0)
    totals = jnp.sum(weights, axis=-1)
    rounded = weights.astype(jnp.bfloat16)
    mixed = jnp.einsum('kgt,tkd->kgd', rounded.astype(jnp.float32), value_rows.astype(jnp.float32)) / totals[..., None]
    return mixed.astype(jnp.bfloat16)


def reference(hidden, request_adapter, adapter_table_row, query_base_weight, down_weight, up_weight, column_scale, rotated_key_cache, cached_value_rows, cache_lengths):
    base_query = jnp.dot(hidden, query_base_weight, preferred_element_type=jnp.float32)
    request_table_rows = adapter_table_row[request_adapter[:, 0]].astype(jnp.int32)
    rank_values = jnp.einsum('gz,czt->gct', hidden.astype(jnp.float32), down_weight.astype(jnp.float32))
    reduced_input = jnp.take_along_axis(rank_values, request_table_rows[:, None, None], axis=1)[:, 0, :].astype(jnp.bfloat16)
    up_weight_rows = up_weight[request_table_rows].astype(jnp.float32)
    adapter_delta = jnp.einsum('nr,nro->no', reduced_input.astype(jnp.float32), up_weight_rows).astype(jnp.bfloat16)
    magnitude = column_scale[request_table_rows].astype(jnp.float32)
    queries = (base_query + adapter_delta.astype(jnp.float32)) * magnitude
    rotated = rotate(queries.reshape(REQUESTS, QUERY_HEADS, HEAD_SIZE), cache_lengths).astype(jnp.bfloat16)
    grouped = rotated.reshape(REQUESTS, KV_HEADS, QUERY_HEADS // KV_HEADS, HEAD_SIZE)
    key_rows = rotated_key_cache.reshape(REQUESTS, CTX, KV_HEADS, HEAD_SIZE)
    value_rows = cached_value_rows.reshape(REQUESTS, CTX, KV_HEADS, HEAD_SIZE)
    outputs = lax.map(attend_one, (grouped, key_rows, value_rows, cache_lengths))
    return outputs.reshape(REQUESTS, QUERY_HEADS * HEAD_SIZE)
```

```python
import functools
import math

import jax
import jax.numpy as jnp
from jax import lax
from jax.experimental import pallas as pl
from jax.experimental.pallas import tpu as pltpu
from jax.sharding import PartitionSpec as P

HEAD_SIZE = 128
CAP = 2
ROPE_BASE = 500000.0
BLOCK_ROWS = 16
GROUP = 8
MESH = pl.DeviceIdType.MESH
LAST = (((1,), (1,)), ((), ()))
F32 = jnp.float32
BF16 = jnp.bfloat16


def iota(shape, dim):
    return lax.broadcasted_iota(jnp.int32, shape, dim)


def kernel(
    owners,
    parts,
    chunks_kv,
    hidden,
    request_adapter,
    table,
    weight,
    down,
    up,
    scale,
    keys,
    values,
    lengths,
    out,
    hid_all,
    w_v,
    down_v,
    up_v,
    scale_v,
    k_v,
    v_v,
    slot_out,
    slot_in,
    scale_out,
    scale_in,
    delta_out,
    delta_in,
    rank_out,
    rank_in,
    q_rows,
    att,
    small_sem,
    w_sem,
    k_sem,
    v_sem,
    slot_send,
    slot_recv,
    scale_send,
    scale_recv,
    delta_send,
    delta_recv,
    hid_send,
    hid_recv,
    rank_send,
    rank_recv,
):
    a = lax.axis_index("adapter")
    t = lax.axis_index("tensor")
    barrier = pltpu.get_barrier_semaphore()
    for d in range(1, owners):
        pl.semaphore_signal(
            barrier, inc=1, device_id=(lax.rem(a + d, owners), t), device_id_type=MESH
        )
    for d in range(1, parts):
        pl.semaphore_signal(
            barrier, inc=1, device_id=(a, lax.rem(t + d, parts)), device_id_type=MESH
        )

    n, feats = hidden.shape
    adapters, rank, columns = up.shape
    slots = adapters * CAP
    chunks = BLOCK_ROWS // slots
    wide_in = feats // chunks
    wide_out = columns // chunks
    lanes = owners * BLOCK_ROWS
    context, kv_width = keys.shape[1], keys.shape[2]
    kv_count = kv_width // HEAD_SIZE
    heads = columns // HEAD_SIZE
    per_kv = heads // kv_count
    row_pad = q_rows.shape[1] // n

    def local(src, dst, sem):
        copy = pltpu.make_async_copy(src, dst, sem)
        copy.start()
        return copy

    hid_copy = local(hidden, hid_all.at[t], small_sem.at[0])
    scale_copy = local(scale, scale_v, small_sem.at[1])
    down_copy = local(
        down.at[:, :, pl.ds(pl.multiple_of(t * feats, 128), feats)], down_v, small_sem.at[2]
    )
    up_copy = local(up, up_v, small_sem.at[3])
    order = [lax.rem(t + d, parts) for d in range(parts)]
    w_copies = [
        local(
            weight.at[pl.ds(pl.multiple_of(order[d] * feats, 128), feats), :],
            w_v.at[d],
            w_sem.at[d],
        )
        for d in range(parts)
    ]
    step = n // chunks_kv
    k_copies = [
        local(keys.at[pl.ds(i * step, step)], k_v.at[pl.ds(i * step, step)], k_sem.at[i])
        for i in range(chunks_kv)
    ]
    v_copies = [
        local(values.at[pl.ds(i * step, step)], v_v.at[pl.ds(i * step, step)], v_sem.at[i])
        for i in range(chunks_kv)
    ]

    side = chunks * n
    rows_n = iota((n, 128), 0)
    row_of = jnp.zeros((n, 128), F32)
    length_of = jnp.zeros((n, 128), F32)
    for i in range(n):
        here = rows_n == i
        row_of = jnp.where(here, table[request_adapter[i]].astype(F32), row_of)
        length_of = jnp.where(here, lengths[i].astype(F32), length_of)
    row_sq = jnp.concatenate([row_of] * chunks, axis=0)
    row_sq_t = jnp.transpose(row_sq)
    r_i = iota((side, side), 0)
    l_i = iota((side, side), 1)
    earlier = (row_sq == row_sq_t) & (l_i < r_i % n)
    repeat = jnp.sum(jnp.where(earlier, 1.0, 0.0), axis=1, keepdims=True)
    slot_col = (row_sq[:, :1] * CAP + repeat).astype(jnp.int32)
    r_i = iota((side, lanes), 0)
    l_i = iota((side, lanes), 1)
    take = (slot_col == (l_i // BLOCK_ROWS) * slots + l_i % slots) & (
        (l_i // slots) % chunks == r_i // n
    )
    unplace = jnp.where(take, 1.0, 0.0)
    place = jnp.transpose(unplace).astype(BF16)
    unplace = unplace.astype(BF16)

    hid_copy.wait()
    own = hid_all[t]
    stacked = jnp.concatenate(
        [own[:, c * wide_in : (c + 1) * wide_in] for c in range(chunks)], axis=0
    )
    slot_out[...] = (
        jnp.dot(place, stacked, preferred_element_type=F32)
        .astype(BF16)
        .reshape(owners, BLOCK_ROWS, wide_in)
    )
    slot_in[a] = slot_out[a]

    pl.semaphore_wait(barrier, owners - 1 + parts - 1)

    def across(d, src, dst, send, recv):
        copy = pltpu.make_async_remote_copy(
            src_ref=src,
            dst_ref=dst,
            send_sem=send.at[d],
            recv_sem=recv.at[d],
            device_id=(lax.rem(a + d, owners), t),
            device_id_type=MESH,
        )
        copy.start()
        return copy

    def beside(d, src, dst, send, recv):
        copy = pltpu.make_async_remote_copy(
            src_ref=src,
            dst_ref=dst,
            send_sem=send.at[d],
            recv_sem=recv.at[d],
            device_id=(a, lax.rem(t + d, parts)),
            device_id_type=MESH,
        )
        copy.start()
        return copy

    slot_copies = [
        across(d, slot_out.at[lax.rem(a + d, owners)], slot_in.at[a], slot_send, slot_recv)
        for d in range(1, owners)
    ]
    hid_copies = [
        beside(d, hid_all.at[t], hid_all.at[t], hid_send, hid_recv) for d in range(1, parts)
    ]

    scale_copy.wait()
    block_row = iota((BLOCK_ROWS, wide_out), 0)
    block = jnp.zeros((BLOCK_ROWS, wide_out), F32)
    scale_f = scale_v[...].astype(F32)
    for c in range(chunks):
        for k in range(adapters):
            piece = scale_f[k : k + 1, c * wide_out : (c + 1) * wide_out]
            at = (block_row // slots == c) & ((block_row % slots) // CAP == k)
            block = jnp.where(at, piece, block)
    scale_out[...] = block.astype(BF16)
    scale_in[a] = scale_out[...]
    scale_copies = [
        across(d, scale_out, scale_in.at[a], scale_send, scale_recv) for d in range(1, owners)
    ]

    lane = iota((n, HEAD_SIZE), 1)
    half = HEAD_SIZE // 2
    frequency = jnp.exp((lane % half).astype(F32) * (-2.0 * math.log(ROPE_BASE) / HEAD_SIZE))
    angles = (length_of - 1.0) * frequency
    cosine = jnp.cos(angles)
    sine = jnp.sin(angles) * jnp.where(lane < half, -1.0, 1.0)
    q_rows[...] = jnp.zeros_like(q_rows)

    def base_part(d, block):
        w_copies[d].wait()
        return jnp.dot(block, w_v[d], preferred_element_type=F32)

    base = base_part(0, own)

    def received(d, copies):
        copies[d - 1].wait_recv()

    m_r = iota((chunks * adapters * rank, lanes), 0)
    m_l = iota((chunks * adapters * rank, lanes), 1)
    mask = (m_r // (adapters * rank) == (m_l // slots) % chunks) & (
        (m_r // rank) % adapters == (m_l % slots) // CAP
    )
    down_copy.wait()
    down_rows = down_v[...].reshape(adapters * rank, feats)
    down_rows = jnp.concatenate(
        [down_rows[:, c * wide_in : (c + 1) * wide_in] for c in range(chunks)], axis=0
    )
    for d in range(1, owners):
        received(d, slot_copies)
    arrived = slot_in[...].reshape(lanes, wide_in)
    products = lax.dot_general(down_rows, arrived, LAST, preferred_element_type=F32)
    products = jnp.where(mask, products, 0.0)
    partial = products[:rank]
    for i in range(1, chunks * adapters):
        partial = partial + products[i * rank : (i + 1) * rank]
    rank_out[...] = partial
    rank_copies = [
        beside(d, rank_out, rank_in.at[t], rank_send, rank_recv) for d in range(1, parts)
    ]
    rank_in[t] = partial

    half_parts = 1 + (parts - 1) // 2
    for d in range(1, half_parts):
        received(d, hid_copies)
        base = base + base_part(parts - d, hid_all[lax.rem(t + parts - d, parts)])

    up_copy.wait()
    up_rows = up_v[...].reshape(adapters * rank, columns)
    up_rows = jnp.concatenate(
        [up_rows[:, c * wide_out : (c + 1) * wide_out] for c in range(chunks)], axis=0
    )
    for d in range(1, parts):
        received(d, rank_copies)
    total = rank_in[0]
    for i in range(1, parts):
        total = total + rank_in[i]
    chunk_of = (iota((rank, lanes), 1) // slots) % chunks
    hop = 1
    while hop < chunks:
        shift = hop * slots
        total = total + jnp.where(
            (chunk_of // hop) % 2 == 0,
            pltpu.roll(total, lanes - shift, 1),
            pltpu.roll(total, shift, 1),
        )
        hop *= 2
    spread = jnp.where(mask, jnp.concatenate([total] * (chunks * adapters), axis=0), 0.0)
    spread = jnp.transpose(spread).astype(BF16)
    delta_out[...] = (
        jnp.dot(spread, up_rows, preferred_element_type=F32)
        .astype(BF16)
        .reshape(owners, BLOCK_ROWS, wide_out)
    )
    delta_copies = [
        across(d, delta_out.at[lax.rem(a + d, owners)], delta_in.at[a], delta_send, delta_recv)
        for d in range(1, owners)
    ]
    delta_in[a] = delta_out[a]

    for d in range(half_parts, parts):
        received(d, hid_copies)
        base = base + base_part(parts - d, hid_all[lax.rem(t + parts - d, parts)])
    for d in range(1, owners):
        received(d, scale_copies)
    magnitude = jnp.dot(
        unplace, scale_in[...].reshape(lanes, wide_out), preferred_element_type=F32
    )
    for copy in k_copies + v_copies:
        copy.wait()
    for d in range(1, owners):
        received(d, delta_copies)
    delta = jnp.dot(unplace, delta_in[...].reshape(lanes, wide_out), preferred_element_type=F32)

    for h in range(heads):
        c, at = divmod(h * HEAD_SIZE, wide_out)
        cut = slice(at, at + HEAD_SIZE)
        query = (
            base[:, h * HEAD_SIZE : (h + 1) * HEAD_SIZE] + delta[c * n : (c + 1) * n, cut]
        ) * magnitude[c * n : (c + 1) * n, cut]
        rotated = query * cosine + pltpu.roll(query, half, 1) * sine
        kv = h // per_kv
        q_rows[kv, pl.ds(h, n, stride=row_pad), :] = rotated

    slot_of = iota((row_pad, context), 1)
    head_row = iota((row_pad, HEAD_SIZE), 0)

    def attend(g, _):
        first = g * GROUP
        scores = []
        for i in range(GROUP):
            at = pl.multiple_of((first + i) * row_pad, 8)
            q = jnp.concatenate(
                [q_rows[kv, pl.ds(at, row_pad), :] for kv in range(kv_count)], axis=1
            ).astype(BF16)
            scores.append(
                lax.dot_general(q, k_v[first + i], LAST, preferred_element_type=F32)
            )
        weights, totals = [], []
        for i in range(GROUP):
            s = jnp.where(slot_of < lengths[first + i], scores[i], -1e30)
            highest = jnp.max(s, axis=1, keepdims=True)
            w = jnp.exp((s - highest) * HEAD_SIZE ** (-0.5))
            totals.append(jnp.sum(w, axis=1, keepdims=True))
            weights.append(w.astype(BF16))
        for i in range(GROUP):
            mixed = jnp.dot(weights[i], v_v[first + i], preferred_element_type=F32)
            picked = mixed[:, :HEAD_SIZE]
            for kv in range(1, kv_count):
                picked = jnp.where(
                    head_row >= kv * per_kv,
                    mixed[:, kv * HEAD_SIZE : (kv + 1) * HEAD_SIZE],
                    picked,
                )
            at = pl.multiple_of((first + i) * row_pad, 8)
            att[pl.ds(at, row_pad), :] = picked / totals[i]
        return 0

    lax.fori_loop(0, n // GROUP, attend, 0)
    for h in range(heads):
        out[:, h * HEAD_SIZE : (h + 1) * HEAD_SIZE] = att[
            pl.ds(h, n, stride=row_pad), :
        ].astype(BF16)
    for copy in slot_copies + scale_copies + delta_copies + hid_copies + rank_copies:
        copy.wait_send()


def shards(
    hidden,
    request_adapter,
    adapter_table_row,
    query_base_weight,
    down_weight,
    up_weight,
    column_scale,
    rotated_key_cache,
    cached_value_rows,
    cache_lengths,
):
    owners = lax.axis_size("adapter")
    parts = lax.axis_size("tensor")
    n, feats = hidden.shape
    adapters, rank, columns = up_weight.shape
    chunks = BLOCK_ROWS // (adapters * CAP)
    lanes = owners * BLOCK_ROWS
    heads = columns // HEAD_SIZE
    row_pad = -(-heads // 8) * 8
    context, kv_width = rotated_key_cache.shape[1:]
    wide_in, wide_out = feats // chunks, columns // chunks
    chunks_kv = 4
    anywhere = pl.BlockSpec(memory_space=pl.ANY)
    scalars = pl.BlockSpec(memory_space=pltpu.SMEM)
    dma = pltpu.SemaphoreType.DMA
    return pl.pallas_call(
        functools.partial(kernel, owners, parts, chunks_kv),
        out_shape=jax.ShapeDtypeStruct((n, columns), BF16),
        in_specs=[anywhere, scalars, scalars] + [anywhere] * 6 + [scalars],
        out_specs=pl.BlockSpec(memory_space=pltpu.VMEM),
        scratch_shapes=[
            pltpu.VMEM((parts, n, feats), BF16),
            pltpu.VMEM((parts, feats, columns), BF16),
            pltpu.VMEM((adapters, rank, feats), BF16),
            pltpu.VMEM((adapters, rank, columns), BF16),
            pltpu.VMEM((adapters, columns), BF16),
            pltpu.VMEM((n, context, kv_width), BF16),
            pltpu.VMEM((n, context, kv_width), BF16),
            pltpu.VMEM((owners, BLOCK_ROWS, wide_in), BF16),
            pltpu.VMEM((owners, BLOCK_ROWS, wide_in), BF16),
            pltpu.VMEM((BLOCK_ROWS, wide_out), BF16),
            pltpu.VMEM((owners, BLOCK_ROWS, wide_out), BF16),
            pltpu.VMEM((owners, BLOCK_ROWS, wide_out), BF16),
            pltpu.VMEM((owners, BLOCK_ROWS, wide_out), BF16),
            pltpu.VMEM((rank, lanes), F32),
            pltpu.VMEM((parts, rank, lanes), F32),
            pltpu.VMEM((kv_width // HEAD_SIZE, n * row_pad, HEAD_SIZE), F32),
            pltpu.VMEM((n * row_pad, HEAD_SIZE), F32),
            dma((4,)),
            dma((parts,)),
            dma((chunks_kv,)),
            dma((chunks_kv,)),
        ]
        + [dma((owners,))] * 6
        + [dma((parts,))] * 4,
        compiler_params=pltpu.CompilerParams(
            collective_id=0, has_side_effects=True, vmem_limit_bytes=60 * 1024 * 1024
        ),
    )(
        hidden,
        request_adapter.reshape(n),
        adapter_table_row,
        query_base_weight,
        jnp.swapaxes(down_weight, 1, 2),
        up_weight,
        column_scale,
        rotated_key_cache,
        cached_value_rows,
        cache_lengths,
    )


def solution(mesh):
    in_specs = (
        P("adapter", "tensor"),
        P("adapter", None),
        P(),
        P(None, "tensor"),
        P("adapter", None, None),
        P("adapter", None, "tensor"),
        P("adapter", "tensor"),
        P("adapter", None, "tensor"),
        P("adapter", None, "tensor"),
        P("adapter"),
    )
    out_specs = P("adapter", "tensor")
    return jax.shard_map(shards, mesh=mesh, in_specs=in_specs, out_specs=out_specs, check_vma=False)
```

```python
import functools
import math

import jax
import jax.numpy as jnp
from jax import lax
from jax.experimental import pallas as pl
from jax.experimental.pallas import tpu as pltpu
from jax.sharding import PartitionSpec as P

HEAD_SIZE = 128
CAP = 2
ROPE_BASE = 500000.0
BLOCK_ROWS = 16
GROUP = 8
MESH = pl.DeviceIdType.MESH
LAST = (((1,), (1,)), ((), ()))
F32 = jnp.float32
BF16 = jnp.bfloat16


def iota(shape, dim):
    return lax.broadcasted_iota(jnp.int32, shape, dim)


def kernel(
    owners,
    parts,
    chunks_kv,
    hidden,
    request_adapter,
    table,
    weight,
    down,
    up,
    scale,
    keys,
    values,
    lengths,
    out,
    hid_all,
    w_v,
    down_v,
    up_v,
    scale_v,
    k_v,
    v_v,
    slot_out,
    slot_in,
    scale_out,
    scale_in,
    delta_out,
    delta_in,
    rank_out,
    rank_in,
    q_rows,
    att,
    small_sem,
    w_sem,
    k_sem,
    v_sem,
    slot_send,
    slot_recv,
    scale_send,
    scale_recv,
    delta_send,
    delta_recv,
    hid_send,
    hid_recv,
    rank_send,
    rank_recv,
):
    a = lax.axis_index("adapter")
    t = lax.axis_index("tensor")
    barrier = pltpu.get_barrier_semaphore()
    for d in range(1, owners):
        pl.semaphore_signal(
            barrier, inc=1, device_id=(lax.rem(a + d, owners), t), device_id_type=MESH
        )
    for d in range(1, parts):
        pl.semaphore_signal(
            barrier, inc=1, device_id=(a, lax.rem(t + d, parts)), device_id_type=MESH
        )

    n, feats = hidden.shape
    adapters, rank, columns = up.shape
    slots = adapters * CAP
    chunks = BLOCK_ROWS // slots
    wide_in = feats // chunks
    wide_out = columns // chunks
    lanes = owners * BLOCK_ROWS
    context, kv_width = keys.shape[1], keys.shape[2]
    kv_count = kv_width // HEAD_SIZE
    heads = columns // HEAD_SIZE
    per_kv = heads // kv_count
    row_pad = q_rows.shape[1] // n

    def local(src, dst, sem):
        copy = pltpu.make_async_copy(src, dst, sem)
        copy.start()
        return copy

    hid_copy = local(hidden, hid_all.at[t], small_sem.at[0])
    scale_copy = local(scale, scale_v, small_sem.at[1])
    down_copy = local(
        down.at[:, :, pl.ds(pl.multiple_of(t * feats, 128), feats)], down_v, small_sem.at[2]
    )
    up_copy = local(up, up_v, small_sem.at[3])
    order = [lax.rem(t + d, parts) for d in range(parts)]
    w_copies = [
        local(
            weight.at[pl.ds(pl.multiple_of(order[d] * feats, 128), feats), :],
            w_v.at[d],
            w_sem.at[d],
        )
        for d in range(parts)
    ]
    step = n // chunks_kv
    k_copies = [
        local(keys.at[pl.ds(i * step, step)], k_v.at[pl.ds(i * step, step)], k_sem.at[i])
        for i in range(chunks_kv)
    ]
    v_copies = [
        local(values.at[pl.ds(i * step, step)], v_v.at[pl.ds(i * step, step)], v_sem.at[i])
        for i in range(chunks_kv)
    ]

    side = chunks * n
    rows_n = iota((n, 128), 0)
    row_of = jnp.zeros((n, 128), F32)
    length_of = jnp.zeros((n, 128), F32)
    for i in range(n):
        here = rows_n == i
        row_of = jnp.where(here, table[request_adapter[i]].astype(F32), row_of)
        length_of = jnp.where(here, lengths[i].astype(F32), length_of)
    row_sq = jnp.concatenate([row_of] * chunks, axis=0)
    row_sq_t = jnp.transpose(row_sq)
    r_i = iota((side, side), 0)
    l_i = iota((side, side), 1)
    earlier = (row_sq == row_sq_t) & (l_i < r_i % n)
    repeat = jnp.sum(jnp.where(earlier, 1.0, 0.0), axis=1, keepdims=True)
    slot_col = (row_sq[:, :1] * CAP + repeat).astype(jnp.int32)
    r_i = iota((side, lanes), 0)
    l_i = iota((side, lanes), 1)
    take = (slot_col == (l_i // BLOCK_ROWS) * slots + l_i % slots) & (
        (l_i // slots) % chunks == r_i // n
    )
    unplace = jnp.where(take, 1.0, 0.0)
    place = jnp.transpose(unplace).astype(BF16)
    unplace = unplace.astype(BF16)

    hid_copy.wait()
    own = hid_all[t]
    stacked = jnp.concatenate(
        [own[:, c * wide_in : (c + 1) * wide_in] for c in range(chunks)], axis=0
    )
    slot_out[...] = (
        jnp.dot(place, stacked, preferred_element_type=F32)
        .astype(BF16)
        .reshape(owners, BLOCK_ROWS, wide_in)
    )
    slot_in[a] = slot_out[a]

    pl.semaphore_wait(barrier, owners - 1 + parts - 1)

    def across(d, src, dst, send, recv):
        copy = pltpu.make_async_remote_copy(
            src_ref=src,
            dst_ref=dst,
            send_sem=send.at[d],
            recv_sem=recv.at[d],
            device_id=(lax.rem(a + d, owners), t),
            device_id_type=MESH,
        )
        copy.start()
        return copy

    def beside(d, src, dst, send, recv):
        copy = pltpu.make_async_remote_copy(
            src_ref=src,
            dst_ref=dst,
            send_sem=send.at[d],
            recv_sem=recv.at[d],
            device_id=(a, lax.rem(t + d, parts)),
            device_id_type=MESH,
        )
        copy.start()
        return copy

    slot_copies = [
        across(d, slot_out.at[lax.rem(a + d, owners)], slot_in.at[a], slot_send, slot_recv)
        for d in range(1, owners)
    ]
    hid_copies = [
        beside(d, hid_all.at[t], hid_all.at[t], hid_send, hid_recv) for d in range(1, parts)
    ]

    scale_copy.wait()
    block_row = iota((BLOCK_ROWS, wide_out), 0)
    block = jnp.zeros((BLOCK_ROWS, wide_out), F32)
    scale_f = scale_v[...].astype(F32)
    for c in range(chunks):
        for k in range(adapters):
            piece = scale_f[k : k + 1, c * wide_out : (c + 1) * wide_out]
            at = (block_row // slots == c) & ((block_row % slots) // CAP == k)
            block = jnp.where(at, piece, block)
    scale_out[...] = block.astype(BF16)
    scale_in[a] = scale_out[...]

    lane = iota((n, HEAD_SIZE), 1)
    half = HEAD_SIZE // 2
    frequency = jnp.exp((lane % half).astype(F32) * (-2.0 * math.log(ROPE_BASE) / HEAD_SIZE))
    angles = (length_of - 1.0) * frequency
    cosine = jnp.cos(angles)
    sine = jnp.sin(angles) * jnp.where(lane < half, -1.0, 1.0)
    q_rows[...] = jnp.zeros_like(q_rows)

    def base_part(d, block):
        w_copies[d].wait()
        return jnp.dot(block, w_v[d], preferred_element_type=F32)

    base = base_part(0, own)

    def received(d, copies):
        copies[d - 1].wait_recv()

    m_r = iota((chunks * adapters * rank, lanes), 0)
    m_l = iota((chunks * adapters * rank, lanes), 1)
    mask = (m_r // (adapters * rank) == (m_l // slots) % chunks) & (
        (m_r // rank) % adapters == (m_l % slots) // CAP
    )
    down_copy.wait()
    down_rows = down_v[...].reshape(adapters * rank, feats)
    down_rows = jnp.concatenate(
        [down_rows[:, c * wide_in : (c + 1) * wide_in] for c in range(chunks)], axis=0
    )
    for d in range(1, owners):
        received(d, slot_copies)
    arrived = slot_in[...].reshape(lanes, wide_in)
    products = lax.dot_general(down_rows, arrived, LAST, preferred_element_type=F32)
    products = jnp.where(mask, products, 0.0)
    partial = products[:rank]
    for i in range(1, chunks * adapters):
        partial = partial + products[i * rank : (i + 1) * rank]
    rank_out[...] = partial
    rank_copies = [
        beside(d, rank_out, rank_in.at[t], rank_send, rank_recv) for d in range(1, parts)
    ]
    scale_copies = [
        across(d, scale_out, scale_in.at[a], scale_send, scale_recv) for d in range(1, owners)
    ]
    rank_in[t] = partial

    half_parts = 1 + (parts - 1) // 2
    for d in range(1, half_parts):
        received(d, hid_copies)
        base = base + base_part(parts - d, hid_all[lax.rem(t + parts - d, parts)])

    up_copy.wait()
    up_rows = up_v[...].reshape(adapters * rank, columns)
    up_rows = jnp.concatenate(
        [up_rows[:, c * wide_out : (c + 1) * wide_out] for c in range(chunks)], axis=0
    )
    for d in range(1, parts):
        received(d, rank_copies)
    total = rank_in[0]
    for i in range(1, parts):
        total = total + rank_in[i]
    chunk_of = (iota((rank, lanes), 1) // slots) % chunks
    hop = 1
    while hop < chunks:
        shift = hop * slots
        total = total + jnp.where(
            (chunk_of // hop) % 2 == 0,
            pltpu.roll(total, lanes - shift, 1),
            pltpu.roll(total, shift, 1),
        )
        hop *= 2
    spread = jnp.where(mask, jnp.concatenate([total] * (chunks * adapters), axis=0), 0.0)
    spread = jnp.transpose(spread).astype(BF16)
    delta_out[...] = (
        jnp.dot(spread, up_rows, preferred_element_type=F32)
        .astype(BF16)
        .reshape(owners, BLOCK_ROWS, wide_out)
    )
    delta_copies = [
        across(d, delta_out.at[lax.rem(a + d, owners)], delta_in.at[a], delta_send, delta_recv)
        for d in range(1, owners)
    ]
    delta_in[a] = delta_out[a]

    for d in range(half_parts, parts):
        received(d, hid_copies)
        base = base + base_part(parts - d, hid_all[lax.rem(t + parts - d, parts)])
    for d in range(1, owners):
        received(d, scale_copies)
    magnitude = jnp.dot(
        unplace, scale_in[...].reshape(lanes, wide_out), preferred_element_type=F32
    )
    for copy in k_copies + v_copies:
        copy.wait()
    for d in range(1, owners):
        received(d, delta_copies)
    delta = jnp.dot(unplace, delta_in[...].reshape(lanes, wide_out), preferred_element_type=F32)

    for h in range(heads):
        c, at = divmod(h * HEAD_SIZE, wide_out)
        cut = slice(at, at + HEAD_SIZE)
        query = (
            base[:, h * HEAD_SIZE : (h + 1) * HEAD_SIZE] + delta[c * n : (c + 1) * n, cut]
        ) * magnitude[c * n : (c + 1) * n, cut]
        rotated = query * cosine + pltpu.roll(query, half, 1) * sine
        kv = h // per_kv
        q_rows[kv, pl.ds(h, n, stride=row_pad), :] = rotated

    slot_of = iota((row_pad, context), 1)
    head_row = iota((row_pad, HEAD_SIZE), 0)

    def attend(g, _):
        first = g * GROUP
        scores = []
        for i in range(GROUP):
            at = pl.multiple_of((first + i) * row_pad, 8)
            q = jnp.concatenate(
                [q_rows[kv, pl.ds(at, row_pad), :] for kv in range(kv_count)], axis=1
            ).astype(BF16)
            scores.append(
                lax.dot_general(q, k_v[first + i], LAST, preferred_element_type=F32)
            )
        weights, totals = [], []
        for i in range(GROUP):
            s = jnp.where(slot_of < lengths[first + i], scores[i], -1e30)
            highest = jnp.max(s, axis=1, keepdims=True)
            w = jnp.exp((s - highest) * HEAD_SIZE ** (-0.5))
            totals.append(jnp.sum(w, axis=1, keepdims=True))
            weights.append(w.astype(BF16))
        for i in range(GROUP):
            mixed = jnp.dot(weights[i], v_v[first + i], preferred_element_type=F32)
            picked = mixed[:, :HEAD_SIZE]
            for kv in range(1, kv_count):
                picked = jnp.where(
                    head_row >= kv * per_kv,
                    mixed[:, kv * HEAD_SIZE : (kv + 1) * HEAD_SIZE],
                    picked,
                )
            at = pl.multiple_of((first + i) * row_pad, 8)
            att[pl.ds(at, row_pad), :] = picked / totals[i]
        return 0

    for g in range(n // GROUP):
        attend(g, 0)
    for h in range(heads):
        out[:, h * HEAD_SIZE : (h + 1) * HEAD_SIZE] = att[
            pl.ds(h, n, stride=row_pad), :
        ].astype(BF16)
    for copy in slot_copies + scale_copies + delta_copies + hid_copies + rank_copies:
        copy.wait_send()


def shards(
    hidden,
    request_adapter,
    adapter_table_row,
    query_base_weight,
    down_weight,
    up_weight,
    column_scale,
    rotated_key_cache,
    cached_value_rows,
    cache_lengths,
):
    owners = lax.axis_size("adapter")
    parts = lax.axis_size("tensor")
    n, feats = hidden.shape
    adapters, rank, columns = up_weight.shape
    chunks = BLOCK_ROWS // (adapters * CAP)
    lanes = owners * BLOCK_ROWS
    heads = columns // HEAD_SIZE
    row_pad = -(-heads // 8) * 8
    context, kv_width = rotated_key_cache.shape[1:]
    wide_in, wide_out = feats // chunks, columns // chunks
    chunks_kv = 4
    anywhere = pl.BlockSpec(memory_space=pl.ANY)
    scalars = pl.BlockSpec(memory_space=pltpu.SMEM)
    dma = pltpu.SemaphoreType.DMA
    return pl.pallas_call(
        functools.partial(kernel, owners, parts, chunks_kv),
        out_shape=pltpu.VMEM((n, columns), BF16),
        in_specs=[anywhere, scalars, scalars] + [anywhere] * 6 + [scalars],
        out_specs=pl.BlockSpec(memory_space=pltpu.VMEM),
        scratch_shapes=[
            pltpu.VMEM((parts, n, feats), BF16),
            pltpu.VMEM((parts, feats, columns), BF16),
            pltpu.VMEM((adapters, rank, feats), BF16),
            pltpu.VMEM((adapters, rank, columns), BF16),
            pltpu.VMEM((adapters, columns), BF16),
            pltpu.VMEM((n, context, kv_width), BF16),
            pltpu.VMEM((n, context, kv_width), BF16),
            pltpu.VMEM((owners, BLOCK_ROWS, wide_in), BF16),
            pltpu.VMEM((owners, BLOCK_ROWS, wide_in), BF16),
            pltpu.VMEM((BLOCK_ROWS, wide_out), BF16),
            pltpu.VMEM((owners, BLOCK_ROWS, wide_out), BF16),
            pltpu.VMEM((owners, BLOCK_ROWS, wide_out), BF16),
            pltpu.VMEM((owners, BLOCK_ROWS, wide_out), BF16),
            pltpu.VMEM((rank, lanes), F32),
            pltpu.VMEM((parts, rank, lanes), F32),
            pltpu.VMEM((kv_width // HEAD_SIZE, n * row_pad, HEAD_SIZE), F32),
            pltpu.VMEM((n * row_pad, HEAD_SIZE), F32),
            dma((4,)),
            dma((parts,)),
            dma((chunks_kv,)),
            dma((chunks_kv,)),
        ]
        + [dma((owners,))] * 6
        + [dma((parts,))] * 4,
        compiler_params=pltpu.CompilerParams(
            collective_id=0, has_side_effects=True, vmem_limit_bytes=60 * 1024 * 1024
        ),
    )(
        hidden,
        request_adapter.reshape(n),
        adapter_table_row,
        query_base_weight,
        jnp.swapaxes(down_weight, 1, 2),
        up_weight,
        column_scale,
        rotated_key_cache,
        cached_value_rows,
        cache_lengths,
    )


def solution(mesh):
    in_specs = (
        P("adapter", "tensor"),
        P("adapter", None),
        P(),
        P(None, "tensor"),
        P("adapter", None, None),
        P("adapter", None, "tensor"),
        P("adapter", "tensor"),
        P("adapter", None, "tensor"),
        P("adapter", None, "tensor"),
        P("adapter"),
    )
    out_specs = P("adapter", "tensor")
    return jax.shard_map(shards, mesh=mesh, in_specs=in_specs, out_specs=out_specs, check_vma=False)
```
